8 devices in a mesh: dp: 2 (over z, y), ep: 4 (over x, core).
Axes of the slice: x: 2, y: 2, z: 1, core: 2. Of those that a mesh axis runs over, the one named last changes fastest.
Arguments:
- tok_x: bfloat16 [8192, 4096], P(('dp', 'ep'))
- tok_dy: bfloat16 [8192, 4096], P(('dp', 'ep'))
- exp_first: int32 [8192], P(('dp', 'ep'))
- exp_second: int32 [8192], P(('dp', 'ep'))
- eligible: int32 [8192, 16], P(('dp', 'ep'))
- slot_first: int32 [8192], P(('dp', 'ep'))
- slot_second: int32 [8192], P(('dp', 'ep'))
- ln_weight: bfloat16 [4096], replicated
- ln_bias: bfloat16 [4096], replicated
- router: bfloat16 [4096, 16], replicated
- w_gate: bfloat16 [16, 4096, 960], P('ep')
- w_up: bfloat16 [16, 4096, 960], P('ep')
- w_down: bfloat16 [16, 960, 4096], P('ep')
Outputs:
- output 1: bfloat16 [8192, 4096], P(('dp', 'ep'))
- output 2: bfloat16 [8192, 4096], P(('dp', 'ep'))
- output 3: float32 [16, 4096, 960], P('ep')
- output 4: float32 [16, 4096, 960], P('ep')
- output 5: float32 [16, 960, 4096], P('ep')
- output 6: float32 [4096, 16], replicated
- output 7: float32 [4096], replicated
- output 8: float32 [4096], replicated
All inputs are finite; a program needn't handle non-finite values.
Results may differ from the reference program's by a relative error of at most 0.00516369.
Values are sent between devices in bfloat16 or wider.
A program may use at most 1.25 GiB of HBM per device.

```python
import jax
import jax.numpy as jnp
from jax import lax

SHARDS = 8
TOK_DEV = 1024
D_MODEL = 4096
FF_DIM = 960
EXPERTS = 16
SLOT_CAP = 192
LN_EPS = 1e-5


def draw_routing(rng_key):
    n_tok = SHARDS * TOK_DEV
    key_list = jax.random.split(rng_key, 5)
    pick_a = jax.random.randint(key_list[0], (n_tok,), 0, EXPERTS)
    pick_b = jax.random.randint(key_list[1], (n_tok,), 0, EXPERTS)
    pick_c = jax.random.randint(key_list[2], (n_tok,), 0, EXPERTS)
    first_pick = jnp.minimum(jnp.minimum(pick_a, pick_b), pick_c)
    second_pick = (first_pick + 1 + jax.random.randint(key_list[3], (n_tok,), 0, EXPERTS - 1)) % EXPERTS
    expert_ids = jnp.arange(EXPERTS)
    hot_first = (first_pick[:, None] == expert_ids[None, :]).astype(jnp.int32)
    hot_second = (second_pick[:, None] == expert_ids[None, :]).astype(jnp.int32)
    extra_bits = (jax.random.randint(key_list[4], (n_tok, EXPERTS), 0, 8) == 0).astype(jnp.int32)
    eligible = jnp.maximum(extra_bits, jnp.maximum(hot_first, hot_second))
    per_first = hot_first.reshape(SHARDS, TOK_DEV, EXPERTS)
    per_second = hot_second.reshape(SHARDS, TOK_DEV, EXPERTS)
    rank_first = jnp.sum((jnp.cumsum(per_first, axis=1) - per_first) * per_first, axis=2).reshape(n_tok)
    used_first = jnp.sum(per_first, axis=1, keepdims=True)
    rank_second = jnp.sum((jnp.cumsum(per_second, axis=1) - per_second + used_first) * per_second, axis=2).reshape(n_tok)
    slot_first = jnp.where(rank_first < SLOT_CAP, rank_first, -1)
    slot_second = jnp.where(rank_second < SLOT_CAP, rank_second, -1)
    return first_pick, second_pick, eligible, slot_first, slot_second


def setup_inputs(seed: int = 0) -> dict:
    key_list = jax.random.split(jax.random.key(seed), 10)
    n_tok = SHARDS * TOK_DEV
    first_pick, second_pick, eligible, slot_first, slot_second = draw_routing(key_list[0])
    tok_x = jax.random.normal(key_list[1], (n_tok, D_MODEL), jnp.float32).astype(jnp.bfloat16)
    tok_dy = jax.random.normal(key_list[2], (n_tok, D_MODEL), jnp.float32).astype(jnp.bfloat16)
    ln_weight = (1.0 + 0.3 * jax.random.normal(key_list[3], (D_MODEL,), jnp.float32)).astype(jnp.bfloat16)
    ln_bias = (0.3 * jax.random.normal(key_list[4], (D_MODEL,), jnp.float32)).astype(jnp.bfloat16)
    router = (1.5 * D_MODEL ** -0.5 * jax.random.normal(key_list[5], (D_MODEL, EXPERTS), jnp.float32)).astype(jnp.bfloat16)
    w_gate = (D_MODEL ** -0.5 * jax.random.normal(key_list[6], (EXPERTS, D_MODEL, FF_DIM), jnp.float32)).astype(jnp.bfloat16)
    w_up = (D_MODEL ** -0.5 * jax.random.normal(key_list[7], (EXPERTS, D_MODEL, FF_DIM), jnp.float32)).astype(jnp.bfloat16)
    w_down = (3.0 * FF_DIM ** -0.5 * jax.random.normal(key_list[8], (EXPERTS, FF_DIM, D_MODEL), jnp.float32)).astype(jnp.bfloat16)
    return {'tok_x': tok_x, 'tok_dy': tok_dy, 'exp_first': first_pick, 'exp_second': second_pick,
            'eligible': eligible, 'slot_first': slot_first, 'slot_second': slot_second,
            'ln_weight': ln_weight, 'ln_bias': ln_bias, 'router': router,
            'w_gate': w_gate, 'w_up': w_up, 'w_down': w_down}


def layer_norm(x_rows, ln_weight, ln_bias):
    x_float = x_rows.astype(jnp.float32)
    centered = x_float - jnp.mean(x_float, axis=-1, keepdims=True)
    inv_std = lax.rsqrt(jnp.mean(centered * centered, axis=-1, keepdims=True) + LN_EPS)
    x_hat = centered * inv_std
    hidden = (x_hat * ln_weight.astype(jnp.float32) + ln_bias.astype(jnp.float32)).astype(jnp.bfloat16)
    return hidden, x_hat, inv_std


def layer_norm_back(grad_h, x_hat, inv_std, ln_weight):
    scaled = grad_h * ln_weight.astype(jnp.float32)
    return inv_std * (scaled - jnp.mean(scaled, axis=-1, keepdims=True)
                      - x_hat * jnp.mean(scaled * x_hat, axis=-1, keepdims=True))


def masked_gate(logits, allowed, choice):
    expert_ids = jnp.arange(logits.shape[-1])
    prob_all = jax.nn.softmax(jnp.where(allowed, logits, -1e30), axis=-1)
    picked = (choice[:, None] == expert_ids[None, :]).astype(jnp.float32)
    return jnp.sum(prob_all * picked, axis=-1), prob_all, picked


def expert_pass(operands):
    hid_rows, grad_rows, gate_w, up_w, down_w = operands
    pre_gate = jnp.dot(hid_rows, gate_w, preferred_element_type=jnp.float32)
    pre_up = jnp.dot(hid_rows, up_w, preferred_element_type=jnp.float32)
    sig_gate = jax.nn.sigmoid(pre_gate)
    silu_gate = pre_gate * sig_gate
    inner_act = (silu_gate * pre_up).astype(jnp.bfloat16)
    exp_out = jnp.dot(inner_act, down_w, preferred_element_type=jnp.float32).astype(jnp.bfloat16)
    grad_inner = jnp.dot(grad_rows, down_w.T, preferred_element_type=jnp.float32)
    grad_pre_gate = (grad_inner * pre_up * sig_gate * (1.0 + pre_gate * (1.0 - sig_gate))).astype(jnp.bfloat16)
    grad_pre_up = (grad_inner * silu_gate).astype(jnp.bfloat16)
    grad_hid = (jnp.dot(grad_pre_gate, gate_w.T, preferred_element_type=jnp.float32)
                + jnp.dot(grad_pre_up, up_w.T, preferred_element_type=jnp.float32)).astype(jnp.bfloat16)
    dw_gate = jnp.dot(hid_rows.T, grad_pre_gate, preferred_element_type=jnp.float32)
    dw_up = jnp.dot(hid_rows.T, grad_pre_up, preferred_element_type=jnp.float32)
    dw_down = jnp.dot(inner_act.T, grad_rows, preferred_element_type=jnp.float32)
    return exp_out, grad_hid, dw_gate, dw_up, dw_down


def reference(tok_x, tok_dy, exp_first, exp_second, eligible, slot_first, slot_second,
              ln_weight, ln_bias, router, w_gate, w_up, w_down):
    n_tok = tok_x.shape[0]
    hidden, x_hat, inv_std = layer_norm(tok_x, ln_weight, ln_bias)
    logits = jnp.dot(hidden, router, preferred_element_type=jnp.float32)
    expert_ids = jnp.arange(EXPERTS)
    allowed = eligible > 0
    gate_one, prob_one, pick_one = masked_gate(logits, allowed, exp_first)
    gate_two, prob_two, pick_two = masked_gate(logits, allowed & (expert_ids[None, :] != exp_first[:, None]), exp_second)
    n_rows = EXPERTS * SHARDS * SLOT_CAP
    shard_idx = jnp.arange(n_tok) // TOK_DEV
    row_one = jnp.where(slot_first >= 0, (exp_first * SHARDS + shard_idx) * SLOT_CAP + slot_first, n_rows)
    row_two = jnp.where(slot_second >= 0, (exp_second * SHARDS + shard_idx) * SLOT_CAP + slot_second, n_rows)
    dy_float = tok_dy.astype(jnp.float32)
    grad_one = (gate_one[:, None] * dy_float).astype(jnp.bfloat16)
    grad_two = (gate_two[:, None] * dy_float).astype(jnp.bfloat16)
    empty_rows = jnp.zeros((n_rows, D_MODEL), jnp.bfloat16)
    hid_buf = empty_rows.at[row_one].set(hidden, mode='drop').at[row_two].set(hidden, mode='drop')
    grad_buf = empty_rows.at[row_one].set(grad_one, mode='drop').at[row_two].set(grad_two, mode='drop')
    exp_out, grad_hid, dw_gate, dw_up, dw_down = lax.map(
        expert_pass,
        (hid_buf.reshape(EXPERTS, SHARDS * SLOT_CAP, D_MODEL), grad_buf.reshape(EXPERTS, SHARDS * SLOT_CAP, D_MODEL),
         w_gate, w_up, w_down))
    exp_out = exp_out.reshape(n_rows, D_MODEL)
    grad_hid = grad_hid.reshape(n_rows, D_MODEL)
    out_one = jnp.take(exp_out, row_one, axis=0, mode='fill', fill_value=0).astype(jnp.float32)
    out_two = jnp.take(exp_out, row_two, axis=0, mode='fill', fill_value=0).astype(jnp.float32)
    y_mix = gate_one[:, None] * out_one + gate_two[:, None] * out_two
    out_tok = (tok_x.astype(jnp.float32) + y_mix).astype(jnp.bfloat16)
    dgate_one = jnp.sum(dy_float * out_one, axis=-1)
    dgate_two = jnp.sum(dy_float * out_two, axis=-1)
    d_logits = ((dgate_one * gate_one)[:, None] * (pick_one - prob_one)
                + (dgate_two * gate_two)[:, None] * (pick_two - prob_two)).astype(jnp.bfloat16)
    d_router = jnp.dot(hidden.T, d_logits, preferred_element_type=jnp.float32)
    grad_h = (jnp.dot(d_logits, router.T, preferred_element_type=jnp.float32)
              + jnp.take(grad_hid, row_one, axis=0, mode='fill', fill_value=0).astype(jnp.float32)
              + jnp.take(grad_hid, row_two, axis=0, mode='fill', fill_value=0).astype(jnp.float32))
    d_ln_weight = jnp.sum(grad_h * x_hat, axis=0)
    d_ln_bias = jnp.sum(grad_h, axis=0)
    dx_tok = (dy_float + layer_norm_back(grad_h, x_hat, inv_std, ln_weight)).astype(jnp.bfloat16)
    return (out_tok, dx_tok, dw_gate, dw_up, dw_down, d_router, d_ln_weight, d_ln_bias)
```

```python
import jax
import jax.numpy as jnp
from jax import lax
from jax.experimental import pallas as pl
from jax.experimental.pallas import tpu as pltpu
from jax.sharding import PartitionSpec as P

LN_EPS = 1e-5
F32, BF16 = jnp.float32, jnp.bfloat16
VMEM_LIMIT = 60 * 1024 * 1024
ROWS, BOTH_COLS = ((1,), (0,)), ((1,), (1,))


def mm(lhs, rhs, dims=ROWS):
    return lax.dot_general(lhs, rhs, (dims, ((), ())), preferred_element_type=F32)


def call(body, grid, in_specs, out_specs, out_shape, operands, flops, scratch=(), aliases=None):
    return pl.pallas_call(
        body, grid=grid, in_specs=in_specs, out_specs=out_specs, out_shape=out_shape, scratch_shapes=list(scratch),
        input_output_aliases=aliases or {},
        compiler_params=pltpu.CompilerParams(vmem_limit_bytes=VMEM_LIMIT,
                                             dimension_semantics=("arbitrary",) * len(grid)),
        cost_estimate=pl.CostEstimate(flops=flops, transcendentals=0, bytes_accessed=flops // 300))(*operands)


def masked_gate(logits, allowed, choice):
    expert_ids = jnp.arange(logits.shape[-1])
    prob_all = jax.nn.softmax(jnp.where(allowed, logits, -1e30), axis=-1)
    picked = (choice[:, None] == expert_ids[None, :]).astype(F32)
    return jnp.sum(prob_all * picked, axis=-1), prob_all, picked


def gather_rows(tokens, tables, gates, n_exp, cap):
    n_src, (n_tok, d_model), tile, step = len(tokens), tokens[0].shape, 512, 256
    n_slot = n_exp * cap
    extra = [] if gates is None else [gates]

    def body(*refs):
        tok_refs, tab_ref = refs[:n_src], refs[n_src]
        out_ref, hot_ref = refs[-2:]

        @pl.when(pl.program_id(0) == 0)
        def _():
            for s in range(n_src):
                ids = lax.broadcasted_iota(jnp.int32, (n_slot, n_tok), 1)
                hot_ref[s] = (ids == tab_ref[:, s:s + 1]).astype(F32).astype(BF16)

        def col(j, carry):
            at = pl.ds(pl.multiple_of(j * step, step), step)
            for s in range(n_src):
                rows = mm(hot_ref[s], tok_refs[s][:, at])
                if extra:
                    rows = rows * refs[n_src + 1][:, s:s + 1]
                out_ref[:, s * cap:(s + 1) * cap, at] = rows.astype(BF16).reshape(n_exp, cap, step)
            return carry

        lax.fori_loop(0, tile // step, col, 0)

    whole = pl.BlockSpec((n_slot, n_src), lambda j: (0, 0))
    return call(body, (d_model // tile,),
                [pl.BlockSpec((n_tok, tile), lambda j: (0, j))] * n_src + [whole] * (1 + len(extra)),
                pl.BlockSpec((n_exp, n_src * cap, tile), lambda j: (0, 0, j)),
                jax.ShapeDtypeStruct((n_exp, n_src * cap, d_model), BF16),
                (*tokens, tables, *extra), 2 * n_src * n_slot * n_tok * d_model,
                [pltpu.VMEM((n_src, n_slot, n_tok), BF16)])


def stack_rows(refs):
    return refs[0][0] if len(refs) == 1 else jnp.concatenate([r[0] for r in refs], axis=0)


def up_pass(h_sets, q_sets, weights, saved=None):
    h_sets, q_sets, saved = list(h_sets or []), list(q_sets or []), list(saved or [])
    n_exp, _, d_model = (h_sets + q_sets)[0].shape
    n_row = sum(v.shape[1] for v in (h_sets or q_sets))
    d_ff, tile = weights[2].shape[1], 2048
    n_h, n_q = len(h_sets), len(q_sets)
    w_in = ([weights[0], weights[1]] if n_h else []) + ([weights[2]] if n_q else [])
    n_out = 3 if n_h else 2

    def body(*refs):
        refs = list(refs)
        take = lambda n: [refs.pop(0) for _ in range(n)]
        h_refs, q_refs, w_refs, saved_refs, outs, accs = take(n_h), take(n_q), take(len(w_in)), take(len(saved)), take(n_out), refs
        k = pl.program_id(1)

        @pl.when(k == 0)
        def _():
            for acc in accs:
                acc[...] = jnp.zeros_like(acc)

        if n_h:
            h = stack_rows(h_refs)
            accs[0][...] += mm(h, w_refs[0][0], BOTH_COLS)
            accs[1][...] += mm(h, w_refs[1][0], BOTH_COLS)
        if n_q:
            accs[-1][...] += mm(stack_rows(q_refs), w_refs[-1][0], BOTH_COLS)

        @pl.when(k == pl.num_programs(1) - 1)
        def _():
            if n_h:
                a, b = accs[0][...], accs[1][...]
                sig = jax.nn.sigmoid(a)
                silu = a * sig
                outs[0][0] = (silu * b).astype(BF16)
                slope = b * sig * (1.0 + a * (1.0 - sig))
            else:
                slope, silu = saved_refs[0][0], saved_refs[1][0]
            if n_q:
                du = accs[-1][...]
                outs[-2][0] = (du * slope).astype(BF16)
                outs[-1][0] = (du * silu).astype(BF16)
            else:
                outs[-2][0] = slope
                outs[-1][0] = silu

    row = lambda v: pl.BlockSpec((1, v.shape[1], tile), lambda e, k: (e, 0, k))
    wide = pl.BlockSpec((1, d_ff, tile), lambda e, k: (e, 0, k))
    act = pl.BlockSpec((1, n_row, d_ff), lambda e, k: (e, 0, 0))
    shape = lambda t: jax.ShapeDtypeStruct((n_exp, n_row, d_ff), t)
    shapes = ([shape(BF16)] if n_h else []) + [shape(BF16 if n_q else F32)] * 2
    return call(body, (n_exp, d_model // tile),
                [row(v) for v in h_sets + q_sets] + [wide] * len(w_in) + [act] * len(saved),
                [act] * n_out, shapes, (*h_sets, *q_sets, *w_in, *saved),
                2 * n_exp * n_row * d_model * d_ff * len(w_in),
                [pltpu.VMEM((n_row, d_ff), F32)] * len(w_in))


def down_pass(inner, d_gate, d_up, weights, cap, picks):
    has_o, has_d = inner is not None, d_gate is not None
    acts = ([inner] if has_o else []) + ([d_gate, d_up] if has_d else [])
    w_in = ([weights[2]] if has_o else []) + ([weights[0], weights[1]] if has_d else [])
    n_exp, _, d_ff = acts[0].shape
    d_model, tile, n_src = weights[2].shape[2], 1024, len(picks)

    def body(*refs):
        refs = list(refs)
        take = lambda n: [refs.pop(0) for _ in range(n)]
        rows = [take(n_src) for _ in acts]
        w_refs = take(len(acts))
        if has_o:
            out = mm(stack_rows(rows[0]), w_refs[0][0]).astype(BF16)
            for s in range(n_src):
                refs.pop(0)[0] = out[s * cap:(s + 1) * cap]
        if has_d:
            back = (mm(stack_rows(rows[-2]), w_refs[-2][0]) + mm(stack_rows(rows[-1]), w_refs[-1][0])).astype(BF16)
            for s in range(n_src):
                refs.pop(0)[0] = back[s * cap:(s + 1) * cap]

    wide = pl.BlockSpec((1, d_ff, tile), lambda e, j: (e, 0, j))
    act = [pl.BlockSpec((1, cap, d_ff), lambda e, j, p=p: (e, p, 0)) for p in picks]
    n_out = n_src * (has_o + has_d)
    return call(body, (n_exp, d_model // tile),
                act * len(acts) + [wide] * len(w_in),
                [pl.BlockSpec((1, cap, tile), lambda e, j: (e, 0, j))] * n_out,
                [jax.ShapeDtypeStruct((n_exp, cap, d_model), BF16)] * n_out,
                (*[a for a in acts for _ in picks], *w_in),
                2 * n_exp * n_src * cap * d_model * d_ff * len(acts))


def weight_grads(h_sets, q_sets, acts, before=None):
    n_exp, _, d_model = h_sets[0].shape
    n_row = sum(v.shape[1] for v in h_sets)
    d_ff, tile = acts[0][0].shape[2], 512
    before = list(before or [])
    n_set, n_grp = len(h_sets), len(acts)

    def body(*refs):
        refs = list(refs)
        take = lambda n: [refs.pop(0) for _ in range(n)]
        h_refs, q_refs, act_refs, prev, outs, act_ref = take(n_set), take(n_set), [take(n_grp) for _ in range(3)], take(len(before)), take(3), refs[0]

        @pl.when(pl.program_id(1) == 0)
        def _():
            for i in range(3):
                at = 0
                for r in act_refs[i]:
                    act_ref[i, :, at:at + r.shape[1]] = r[0].T
                    at += r.shape[1]

        h, q = stack_rows(h_refs), stack_rows(q_refs)
        for i, rows in ((0, q), (1, h), (2, h)):
            total = mm(act_ref[i], rows)
            outs[i][0] = prev[i][0] + total if prev else total

    row = lambda v: pl.BlockSpec((1, v.shape[1], tile), lambda e, i: (e, 0, i))
    act = lambda v: pl.BlockSpec((1, v.shape[1], d_ff), lambda e, i: (e, 0, 0))
    wide = pl.BlockSpec((1, d_ff, tile), lambda e, i: (e, 0, i))
    flat = [grp[i] for i in range(3) for grp in acts]
    return call(body, (n_exp, d_model // tile),
                [row(v) for v in (*h_sets, *q_sets)] + [act(v) for v in flat] + [wide] * len(before), [wide] * 3,
                [jax.ShapeDtypeStruct((n_exp, d_ff, d_model), F32)] * 3,
                (*h_sets, *q_sets, *flat, *before), 6 * n_exp * n_row * d_model * d_ff,
                [pltpu.VMEM((3, d_ff, n_row), BF16)],
                {2 * n_set + 3 * n_grp + i: i for i in range(3)} if before else None)


def one_hot(pos, n_slot):
    return (lax.broadcasted_iota(jnp.int32, (pos.shape[0], n_slot), 1) == pos).astype(F32).astype(BF16)


def combine_out(blocks, pos, gates, base, tok_dy, dg_base=None):
    n_blk = len(blocks)
    n_exp, cap, d_model = blocks[0].shape
    n_tok, tile, step = tok_dy.shape[0], 512, 256
    n_slot = n_exp * cap
    extra = [] if dg_base is None else [dg_base]

    def body(*refs):
        blk = refs[:n_blk]
        pos_ref, gate_ref, base_ref, dy_ref = refs[n_blk:n_blk + 4]
        out_ref, dg_ref, hot_one, hot_two = refs[-4:]

        @pl.when(pl.program_id(0) == 0)
        def _():
            dg_ref[...] = refs[n_blk + 4][...] if extra else jnp.zeros_like(dg_ref)
            for f in range(n_blk):
                hot_one[f] = one_hot(pos_ref[:, f:f + 1], n_slot)
                hot_two[f] = one_hot(pos_ref[:, n_blk + f:n_blk + f + 1], n_slot)

        def col(j, carry):
            at = pl.ds(pl.multiple_of(j * step, step), step)
            o_one = sum(mm(hot_one[f], blk[f][:, :, at].reshape(n_slot, step)) for f in range(n_blk))
            o_two = sum(mm(hot_two[f], blk[f][:, :, at].reshape(n_slot, step)) for f in range(n_blk))
            dy = dy_ref[:, at].astype(F32)
            mix = gate_ref[:, 0:1] * o_one + gate_ref[:, 1:2] * o_two
            out_ref[:, at] = (base_ref[:, at].astype(F32) + mix).astype(out_ref.dtype)
            dg_ref[:, 0:1] += jnp.sum(dy * o_one, axis=1, keepdims=True)
            dg_ref[:, 1:2] += jnp.sum(dy * o_two, axis=1, keepdims=True)
            return carry

        lax.fori_loop(0, tile // step, col, 0)

    tok = pl.BlockSpec((n_tok, tile), lambda j: (0, j))
    small = lambda n: pl.BlockSpec((n_tok, n), lambda j: (0, 0))
    return call(body, (d_model // tile,),
                [pl.BlockSpec((n_exp, cap, tile), lambda j: (0, 0, j))] * n_blk + [small(2 * n_blk), small(2), tok, tok]
                + [small(2)] * len(extra), [tok, small(2)],
                [jax.ShapeDtypeStruct((n_tok, d_model), BF16 if extra else F32), jax.ShapeDtypeStruct((n_tok, 2), F32)],
                (*blocks, pos, gates, base, tok_dy, *extra), 4 * n_tok * n_blk * n_slot * d_model,
                [pltpu.VMEM((n_blk, n_tok, n_slot), BF16)] * 2)


def pair_hot(hot_ref, pos_ref, n_blk, n_slot):
    for f in range(n_blk):
        hot_ref[f] = (one_hot(pos_ref[:, f:f + 1], n_slot)
                      + one_hot(pos_ref[:, n_blk + f:n_blk + f + 1], n_slot))


def combine_part(blocks, pos):
    n_blk = len(blocks)
    n_exp, cap, d_model = blocks[0].shape
    n_tok, tile, step = pos.shape[0], 512, 256
    n_slot = n_exp * cap

    def body(*refs):
        blk, (pos_ref, out_ref, hot_ref) = refs[:n_blk], refs[n_blk:]

        @pl.when(pl.program_id(0) == 0)
        def _():
            pair_hot(hot_ref, pos_ref, n_blk, n_slot)

        def col(j, carry):
            at = pl.ds(pl.multiple_of(j * step, step), step)
            out_ref[:, at] = sum(mm(hot_ref[f], blk[f][:, :, at].reshape(n_slot, step)) for f in range(n_blk))
            return carry

        lax.fori_loop(0, tile // step, col, 0)

    return call(body, (d_model // tile,),
                [pl.BlockSpec((n_exp, cap, tile), lambda j: (0, 0, j))] * n_blk + [pl.BlockSpec((n_tok, 2 * n_blk), lambda j: (0, 0))],
                pl.BlockSpec((n_tok, tile), lambda j: (0, j)), jax.ShapeDtypeStruct((n_tok, d_model), F32),
                (*blocks, pos), 2 * n_tok * n_blk * n_slot * d_model, [pltpu.VMEM((n_blk, n_tok, n_slot), BF16)])


def combine_back(blocks, pos, part, tok_x, tok_dy, stats, d_logits, router, ln_weight):
    n_blk = len(blocks)
    n_exp, cap, d_model = blocks[0].shape
    n_tok, tile, step = tok_x.shape[0], 512, 256
    n_slot, n_tile = n_exp * cap, d_model // 512

    def body(*refs):
        blk = refs[:n_blk]
        (pos_ref, part_ref, x_ref, dy_ref, stat_ref, dl_ref, rt_ref, lnw_ref,
         dx_ref, dw_ref, db_ref, hot_ref, gh_ref, m1_ref, m2_ref) = refs[n_blk:]
        phase, j = pl.program_id(0), pl.program_id(1)

        @pl.when((phase == 0) & (j == 0))
        def _():
            m1_ref[...] = jnp.zeros_like(m1_ref)
            m2_ref[...] = jnp.zeros_like(m2_ref)
            pair_hot(hot_ref, pos_ref, n_blk, n_slot)

        @pl.when(phase == 0)
        def _():
            def col(i, carry):
                at = pl.ds(pl.multiple_of(i * step, step), step)
                grad = sum(mm(hot_ref[f], blk[f][:, :, at].reshape(n_slot, step)) for f in range(n_blk))
                grad = mm(dl_ref[...], rt_ref[:, at]) + (part_ref[:, at] + grad)
                gh_ref[j, :, at] = grad
                x_hat = (x_ref[:, at].astype(F32) - stat_ref[:, 0:1]) * stat_ref[:, 1:2]
                scaled = grad * lnw_ref[:, at].astype(F32)
                m1_ref[...] += jnp.sum(scaled, axis=1, keepdims=True)
                m2_ref[...] += jnp.sum(scaled * x_hat, axis=1, keepdims=True)
                dw_ref[:, at] = jnp.sum(grad * x_hat, axis=0, keepdims=True)
                db_ref[:, at] = jnp.sum(grad, axis=0, keepdims=True)
                return carry

            lax.fori_loop(0, tile // step, col, 0)

        @pl.when(phase == 1)
        def _():
            x_hat = (x_ref[...].astype(F32) - stat_ref[:, 0:1]) * stat_ref[:, 1:2]
            scaled = gh_ref[j] * lnw_ref[...].astype(F32)
            d_ln = stat_ref[:, 1:2] * (scaled - m1_ref[...] / d_model - x_hat * (m2_ref[...] / d_model))
            dx_ref[...] = (dy_ref[...].astype(F32) + d_ln).astype(BF16)

    last = n_tile - 1
    early = lambda p, j: j * (1 - p) + last * p
    tok = pl.BlockSpec((n_tok, tile), lambda p, j: (0, j))
    tok_early = pl.BlockSpec((n_tok, tile), lambda p, j: (0, early(p, j)))
    tok_late = pl.BlockSpec((n_tok, tile), lambda p, j: (0, j * p))
    wide = lambda n: pl.BlockSpec((n, tile), lambda p, j: (0, j))
    wide_early = lambda n: pl.BlockSpec((n, tile), lambda p, j: (0, early(p, j)))
    small = lambda n: pl.BlockSpec((n_tok, n), lambda p, j: (0, 0))
    return call(body, (2, n_tile),
                [pl.BlockSpec((n_exp, cap, tile), lambda p, j: (0, 0, early(p, j)))] * n_blk
                + [small(2 * n_blk), tok_early, tok, tok_late, small(2), small(router.shape[0]), wide(router.shape[0]), wide(1)],
                [tok_late, wide_early(1), wide_early(1)],
                [jax.ShapeDtypeStruct((n_tok, d_model), BF16)] + [jax.ShapeDtypeStruct((1, d_model), F32)] * 2,
                (*blocks, pos, part, tok_x, tok_dy, stats, d_logits, router, ln_weight), 2 * n_tok * n_blk * n_slot * d_model,
                [pltpu.VMEM((n_blk, n_tok, n_slot), BF16), pltpu.VMEM((n_tile, n_tok, tile), F32)]
                + [pltpu.VMEM((n_tok, 1), F32)] * 2)


def solution(mesh):
    n_dp, n_ep = mesh.shape['dp'], mesh.shape['ep']
    tok_spec = P(('dp', 'ep'), None)
    row_spec = P(('dp', 'ep'))
    exp_spec = P('ep', None, None)

    def swap(value, flip_dp, flip_ep):
        pairs = [(d * n_ep + e, (d ^ flip_dp) * n_ep + (e ^ flip_ep)) for d in range(n_dp) for e in range(n_ep)]
        return lax.ppermute(value, ('dp', 'ep'), pairs)

    def local_step(tok_x, tok_dy, exp_first, exp_second, eligible, slot_first, slot_second,
                   ln_weight, ln_bias, router, w_gate, w_up, w_down):
        n_local, _ = tok_x.shape
        n_exp = eligible.shape[1]
        local_exp = w_gate.shape[0]
        cap = 3 * n_local // n_exp
        n_slot = local_exp * cap
        me = lax.axis_index('ep')
        weights = (jnp.swapaxes(w_gate, 1, 2), jnp.swapaxes(w_up, 1, 2), w_down)

        x_float = tok_x.astype(F32)
        mean = jnp.mean(x_float, axis=-1, keepdims=True)
        centered = x_float - mean
        inv_std = lax.rsqrt(jnp.mean(centered * centered, axis=-1, keepdims=True) + LN_EPS)
        hidden = (centered * inv_std * ln_weight.astype(F32) + ln_bias.astype(F32)).astype(BF16)
        logits = jnp.dot(hidden, router, preferred_element_type=F32)
        expert_ids = jnp.arange(n_exp)
        allowed = eligible > 0
        gate_one, prob_one, pick_one = masked_gate(logits, allowed, exp_first)
        gate_two, prob_two, pick_two = masked_gate(logits, allowed & (expert_ids[None, :] != exp_first[:, None]), exp_second)
        pos_one = jnp.where(slot_first >= 0, exp_first * cap + slot_first, -1)
        pos_two = jnp.where(slot_second >= 0, exp_second * cap + slot_second, -1)
        row_ids = jnp.arange(n_exp * cap)
        hit_one = pos_one[:, None] == row_ids[None, :]
        hit_two = pos_two[:, None] == row_ids[None, :]
        slot_tok = jnp.max(jnp.where(hit_one | hit_two, jnp.arange(n_local)[:, None], -1), axis=0).astype(F32)
        slot_gate = jnp.sum(jnp.where(hit_one, gate_one[:, None], 0.0) + jnp.where(hit_two, gate_two[:, None], 0.0), axis=0)
        meta = jnp.stack([slot_tok, slot_gate])

        def columns(*tables):
            mine = [lax.dynamic_slice(t, (0, me * n_slot), (2, n_slot)) for t in tables]
            both = jnp.stack(mine, axis=-1)
            return both[0].astype(jnp.int32), both[1]

        def spread(value):
            from_x = swap(value, 0, 2)
            from_y = swap(value, 1, 0)
            from_d = swap(from_x, 1, 0)
            return [(v, swap(v, 0, 1)) for v in
                    (value, from_x, from_y, from_d)]

        (m_a, m_x, m_y, m_d) = spread(meta)
        (h_a, h_x, h_y, h_d) = spread(hidden)
        (g_a, g_x, g_y, g_d) = spread(tok_dy)

        def gath(toks, tables, gated):
            tab, gts = columns(*tables)
            return gather_rows(toks, tab, gts if gated else None, local_exp, cap)

        ha, qa = [gath(h_a, m_a, False)], [gath(g_a, m_a, True)]
        act_a = up_pass(ha, qa, weights)
        o_a0, o_a1, b_a0, b_a1 = down_pass(*act_a, weights, cap, (0, 1))
        m_p, m_r = (m_x[0], m_y[0]), (m_x[1], m_y[1])
        hxy = [gath((h_x[0], h_y[0]), m_p, False), gath((h_x[1], h_y[1]), m_r, False)]
        u_xy, *slopes = up_pass(hxy, None, weights)
        o_x0, o_x1 = down_pass(u_xy, None, None, weights, cap, (0, 2))
        qxy = [gath((g_x[0], g_y[0]), m_p, True), gath((g_x[1], g_y[1]), m_r, True)]
        d_xy = up_pass(None, qxy, weights, slopes)
        b_x0, b_x1 = down_pass(None, *d_xy, weights, cap, (0, 2))
        part = weight_grads(hxy, qxy, [(u_xy, *d_xy)])
        hd = [gath(h_d[i:i + 1], m_d[i:i + 1], False) for i in range(2)]
        u_d, *slopes = up_pass(hd, None, weights)
        qd = [gath(g_d[i:i + 1], m_d[i:i + 1], True) for i in range(2)]
        d_d = up_pass(None, qd, weights, slopes)
        dw_down, dw_gate, dw_up = weight_grads(ha + hd, qa + qd, [act_a, (u_d, *d_d)], part)

        outs = [o_a0, swap(o_a1, 0, 1), swap(o_x0, 0, 2), swap(o_x1, 0, 3)]
        backs = [b_a0, swap(b_a1, 0, 1), swap(b_x0, 0, 2), swap(b_x1, 0, 3)]

        def slots(flips):
            cols = [(p, p - (me ^ f) * n_slot) for p in (pos_one, pos_two) for f in flips]
            return jnp.stack([jnp.where(p < 0, -1, at) for p, at in cols], axis=-1)

        near, far = slots((0, 1)), slots((2, 3))
        gates = jnp.stack([gate_one, gate_two], axis=-1)
        mix, dgate = combine_out(outs[:2], near, gates, tok_x, tok_dy)
        out_tok, dgate = combine_out(outs[2:], far, gates, mix, tok_dy, dgate)
        d_logits = ((dgate[:, 0] * gate_one)[:, None] * (pick_one - prob_one)
                    + (dgate[:, 1] * gate_two)[:, None] * (pick_two - prob_two)).astype(BF16)
        d_router = jnp.einsum('te,td->ed', d_logits, hidden, preferred_element_type=F32)

        def sum_all(value):
            for flips in ((0, 1), (1, 0), (0, 2)):
                value = value + swap(value, *flips)
            return value

        d_router = sum_all(d_router)
        part_back = combine_part(backs[:2], near)
        dx_tok, d_lnw, d_lnb = combine_back(backs[2:], far, part_back, tok_x, tok_dy,
                                            jnp.concatenate([mean, inv_std], axis=1), d_logits, router.T, ln_weight[None, :])
        d_ln = sum_all(jnp.concatenate([d_lnw, d_lnb], axis=0))
        return (out_tok, dx_tok, jnp.swapaxes(dw_gate, 1, 2), jnp.swapaxes(dw_up, 1, 2), dw_down, d_router.T, d_ln[0], d_ln[1])

    return jax.shard_map(
        local_step, mesh=mesh,
        in_specs=(tok_spec, tok_spec, row_spec, row_spec, tok_spec, row_spec, row_spec,
                  P(), P(), P(), exp_spec, exp_spec, exp_spec),
        out_specs=(tok_spec, tok_spec, exp_spec, exp_spec, exp_spec, P(), P(), P()),
        check_vma=False)
```

```python
import jax
import jax.numpy as jnp
from jax import lax
from jax.experimental import pallas as pl
from jax.experimental.pallas import tpu as pltpu
from jax.sharding import PartitionSpec as P

LN_EPS = 1e-5
F32, BF16 = jnp.float32, jnp.bfloat16
VMEM_LIMIT = 60 * 1024 * 1024
ROWS, BOTH_COLS = ((1,), (0,)), ((1,), (1,))


def mm(lhs, rhs, dims=ROWS):
    return lax.dot_general(lhs, rhs, (dims, ((), ())), preferred_element_type=F32)


def call(body, grid, in_specs, out_specs, out_shape, operands, flops, scratch=(), aliases=None):
    return pl.pallas_call(
        body, grid=grid, in_specs=in_specs, out_specs=out_specs, out_shape=out_shape, scratch_shapes=list(scratch),
        input_output_aliases=aliases or {},
        compiler_params=pltpu.CompilerParams(vmem_limit_bytes=VMEM_LIMIT,
                                             dimension_semantics=("arbitrary",) * len(grid)),
        cost_estimate=pl.CostEstimate(flops=flops, transcendentals=0, bytes_accessed=flops // 300))(*operands)


def masked_gate(logits, allowed, choice):
    expert_ids = jnp.arange(logits.shape[-1])
    prob_all = jax.nn.softmax(jnp.where(allowed, logits, -1e30), axis=-1)
    picked = (choice[:, None] == expert_ids[None, :]).astype(F32)
    return jnp.sum(prob_all * picked, axis=-1), prob_all, picked


def gather_rows(tokens, tables, gates, n_exp, cap, into=None, shape=None, row_at=0, col_at=0, after=None):
    n_src, n_part, n_tok = len(tokens), len(tokens[0]), tokens[0][0].shape[0]
    n_col = sum(v.shape[1] for v in tokens[0])
    tile = 512 if n_part > 1 or n_col % 1024 else 1024
    n_slot = n_exp * cap
    extra = [] if gates is None else [gates]
    flat = [v for parts in tokens for v in parts]
    rest = [v for v in (into, after) if v is not None]

    def body(*refs):
        tab_ref, (out_ref, hot_ref) = refs[len(flat)], refs[-2:]

        @pl.when(pl.program_id(0) == 0)
        def _():
            ids = lax.broadcasted_iota(jnp.int32, (n_slot, n_tok), 1)
            for s in range(n_src):
                hot_ref[s] = (ids == tab_ref[:, s:s + 1]).astype(F32).astype(BF16)

        def emit(part):
            for s in range(n_src):
                rows = mm(hot_ref[s], refs[s * n_part + part][...])
                if extra:
                    rows = rows * refs[len(flat) + 1][:, s:s + 1]
                out_ref[:, s * cap:(s + 1) * cap, :] = rows.astype(BF16).reshape(n_exp, cap, tile)

        if n_part == 1:
            emit(0)
        else:
            pl.when(pl.program_id(0) == 0)(lambda: emit(0))
            pl.when(pl.program_id(0) > 0)(lambda: emit(1))

    maps = [lambda j: (0, j)] if n_part == 1 else [lambda j: (0, 0), lambda j: (0, jnp.maximum(j - 1, 0))]
    whole = pl.BlockSpec((n_slot, n_src), lambda j: (0, 0))
    return call(body, (n_col // tile,),
                [pl.BlockSpec((n_tok, tile), m) for _ in tokens for m in maps] + [whole] * (1 + len(extra))
                + [pl.BlockSpec(memory_space=pl.ANY)] * len(rest),
                pl.BlockSpec((n_exp, n_src * cap, tile), lambda j: (0, row_at, j + col_at)),
                jax.ShapeDtypeStruct(shape or (n_exp, n_src * cap, n_col), BF16),
                (*flat, tables, *extra, *rest), 2 * n_src * n_slot * n_tok * n_col,
                [pltpu.VMEM((n_src, n_slot, n_tok), BF16)],
                None if into is None else {len(flat) + 1 + len(extra): 0})


def late_pass(q_rows, w_down, n_first, slopes=None, part=None):
    n_exp, n_row, d_model = q_rows.shape
    d_ff, tile = w_down.shape[1], 512
    n_col = d_model if slopes is None else n_first

    def body(q_ref, w_ref, *refs):
        if slopes is None:
            refs[0][0] = mm(q_ref[0, :, n_first:], w_ref[0, :, n_first:], BOTH_COLS)
        else:
            du = refs[2][0] + mm(q_ref[0], w_ref[0], BOTH_COLS)
            for k in range(2):
                refs[3 + k][0] = (du * refs[k][0]).astype(BF16).T

    act = pl.BlockSpec((1, n_row, tile), lambda e, k: (e, 0, k))
    turn = pl.BlockSpec((1, tile, n_row), lambda e, k: (e, k, 0))
    more = [] if slopes is None else [*slopes, part]
    return call(body, (n_exp, pl.cdiv(d_ff, tile)),
                [pl.BlockSpec((1, n_row, n_col), lambda e, k: (e, 0, 0)), pl.BlockSpec((1, tile, n_col), lambda e, k: (e, k, 0))]
                + [act] * len(more), [turn] * 2 if more else act,
                [jax.ShapeDtypeStruct((n_exp, d_ff, n_row), BF16)] * 2 if more else jax.ShapeDtypeStruct((n_exp, n_row, d_ff), F32),
                (q_rows, w_down, *more), 2 * n_exp * n_row * n_col * d_ff)


def stack_rows(refs):
    return refs[0][0] if len(refs) == 1 else jnp.concatenate([r[0] for r in refs], axis=0)


def up_pass(h_sets, q_sets, weights, saved=None, plain=True):
    h_sets, q_sets, saved = list(h_sets or []), list(q_sets or []), list(saved or [])
    sets = h_sets or q_sets
    groups = [[i] for i in range(len(sets))] if sets[0].shape[1] >= 256 else [list(range(len(sets)))]
    n_exp, _, d_model = sets[0].shape
    n_row = sum(v.shape[1] for v in sets)
    d_ff, tile = weights[2].shape[1], 512
    n_h, n_q = len(h_sets), len(q_sets)
    w_in = ([weights[0], weights[1]] if n_h else []) + ([weights[2]] if n_q else [])
    n_half = (1 if n_h else 0) + (2 if n_q else 0)
    n_slope = 0 if n_q else 2

    def body(*refs):
        refs = list(refs)
        take = lambda n: [refs.pop(0) for _ in range(n)]
        h_refs, q_refs, w_refs, saved_refs = take(n_h), take(n_q), take(len(w_in)), take(len(saved))
        flat, turned, slopes = take(n_half if plain else 0), take(n_half), take(n_slope)
        at = 0
        for group in groups:
            size = sum(sets[i].shape[1] for i in group)
            rows = pl.ds(at, size)
            at += size
            halves = []
            if n_h:
                h = stack_rows([h_refs[i] for i in group])
                a = mm(h, w_refs[0][0], BOTH_COLS)
                b = mm(h, w_refs[1][0], BOTH_COLS)
                sig = jax.nn.sigmoid(a)
                silu = a * sig
                halves.append(silu * b)
                slope = b * sig * (1.0 + a * (1.0 - sig))
            else:
                slope, silu = saved_refs[0][0, rows], saved_refs[1][0, rows]
            if n_q:
                du = mm(stack_rows([q_refs[i] for i in group]), w_refs[-1][0], BOTH_COLS)
                halves += [du * slope, du * silu]
            else:
                slopes[0][0, rows] = slope
                slopes[1][0, rows] = silu
            for n, value in enumerate(halves):
                value = value.astype(BF16)
                if plain:
                    flat[n][0, rows] = value
                turned[n][0, :, rows] = value.T

    row = lambda v: pl.BlockSpec((1, v.shape[1], d_model), lambda e, k: (e, 0, 0))
    wide = pl.BlockSpec((1, tile, d_model), lambda e, k: (e, k, 0))
    act = pl.BlockSpec((1, n_row, tile), lambda e, k: (e, 0, k))
    turn = pl.BlockSpec((1, tile, n_row), lambda e, k: (e, k, 0))
    n_flat = n_half if plain else 0
    out = call(body, (n_exp, pl.cdiv(d_ff, tile)),
               [row(v) for v in h_sets + q_sets] + [wide] * len(w_in) + [act] * len(saved),
               [act] * n_flat + [turn] * n_half + [act] * n_slope,
               [jax.ShapeDtypeStruct((n_exp, n_row, d_ff), BF16)] * n_flat + [jax.ShapeDtypeStruct((n_exp, d_ff, n_row), BF16)] * n_half
               + [jax.ShapeDtypeStruct((n_exp, n_row, d_ff), F32)] * n_slope, (*h_sets, *q_sets, *w_in, *saved),
               2 * n_exp * n_row * d_model * d_ff * len(w_in))
    return out[:n_flat], out[n_flat:n_flat + n_half], out[n_flat + n_half:]


def down_pass(inner, d_gate, d_up, weights, cap, picks):
    has_o, has_d = inner is not None, d_gate is not None
    acts = ([inner] if has_o else []) + ([d_gate, d_up] if has_d else [])
    w_in = ([weights[2]] if has_o else []) + ([weights[0], weights[1]] if has_d else [])
    n_exp, _, d_ff = acts[0].shape
    d_model, tile, n_src = weights[2].shape[2], 2048, len(picks)

    def body(*refs):
        refs = list(refs)
        take = lambda n: [refs.pop(0) for _ in range(n)]
        rows = [take(n_src) for _ in acts]
        w_refs = take(len(acts))
        if has_o:
            out = mm(stack_rows(rows[0]), w_refs[0][0]).astype(BF16)
            for s in range(n_src):
                refs.pop(0)[0] = out[s * cap:(s + 1) * cap]
        if has_d:
            back = (mm(stack_rows(rows[-2]), w_refs[-2][0]) + mm(stack_rows(rows[-1]), w_refs[-1][0])).astype(BF16)
            for s in range(n_src):
                refs.pop(0)[0] = back[s * cap:(s + 1) * cap]

    wide = pl.BlockSpec((1, d_ff, tile), lambda e, j: (e, 0, j))
    act = [pl.BlockSpec((1, cap, d_ff), lambda e, j, p=p: (e, p, 0)) for p in picks]
    n_out = n_src * (has_o + has_d)
    return call(body, (n_exp, d_model // tile),
                act * len(acts) + [wide] * len(w_in),
                [pl.BlockSpec((1, cap, tile), lambda e, j: (e, 0, j))] * n_out,
                [jax.ShapeDtypeStruct((n_exp, cap, d_model), BF16)] * n_out,
                (*[a for a in acts for _ in picks], *w_in),
                2 * n_exp * n_src * cap * d_model * d_ff * len(acts))


def weight_grads(jobs, tile):
    n_exp, _, d_model = jobs[0][1][0].shape
    d_ff = jobs[0][0][0].shape[1]
    operands, specs, where, shared = [], [], [], {}

    def put(value, spec):
        if id(value) not in shared:
            shared[id(value)] = len(operands)
            operands.append(value)
            specs.append(spec)
        return shared[id(value)]

    row = lambda v: pl.BlockSpec((1, v.shape[1], tile), lambda e, i: (e, 0, i))
    act = lambda v: pl.BlockSpec((1, d_ff, v.shape[2]), lambda e, i: (e, 0, 0))
    wide = pl.BlockSpec((1, d_ff, tile), lambda e, i: (e, 0, i))
    aliases = {}
    for n, (acts, rows, before) in enumerate(jobs):
        at = [put(v, act(v)) for v in acts], [put(v, row(v)) for v in rows], None if before is None else put(before, wide)
        where.append(at)
        if before is not None:
            aliases[at[2]] = n
    n_rows = [sum(v.shape[1] for v in rows) for _, rows, _ in jobs]

    def body(*refs):
        ins, outs = refs[:len(operands)], refs[len(operands):]
        for (acts, rows, before), out in zip(where, outs):
            total = mm(jnp.concatenate([ins[r][0] for r in acts], axis=1), stack_rows([ins[r] for r in rows]))
            out[0] = total if before is None else ins[before][0] + total

    return call(body, (n_exp, d_model // tile), specs, [wide] * len(jobs),
                [jax.ShapeDtypeStruct((n_exp, d_ff, d_model), F32)] * len(jobs), operands,
                2 * n_exp * sum(n_rows) * d_model * d_ff, (), aliases)


def lane_sums(value):
    return sum(value[:, i:i + 128] for i in range(0, value.shape[1], 128))


def one_hot(pos, n_slot):
    return (lax.broadcasted_iota(jnp.int32, (pos.shape[0], n_slot), 1) == pos).astype(F32).astype(BF16)


def combine_out(blocks, pos, gates, base, tok_dy, dg_base=None):
    n_blk = len(blocks)
    n_exp, cap, d_model = blocks[0].shape
    n_tok, tile, step = tok_dy.shape[0], 512, 256
    n_slot = n_exp * cap
    extra = [] if dg_base is None else [dg_base]

    def body(*refs):
        blk = refs[:n_blk]
        pos_ref, gate_ref, base_ref, dy_ref = refs[n_blk:n_blk + 4]
        out_ref, dg_ref, hot_one, hot_two, sum_one, sum_two = refs[-6:]

        @pl.when(pl.program_id(0) == 0)
        def _():
            sum_one[...] = jnp.zeros_like(sum_one)
            sum_two[...] = jnp.zeros_like(sum_two)
            for f in range(n_blk):
                hot_one[f] = one_hot(pos_ref[:, f:f + 1], n_slot)
                hot_two[f] = one_hot(pos_ref[:, n_blk + f:n_blk + f + 1], n_slot)

        def col(j):
            at = pl.ds(j * step, step)
            o_one = sum(mm(hot_one[f], blk[f][:, :, at].reshape(n_slot, step)) for f in range(n_blk))
            o_two = sum(mm(hot_two[f], blk[f][:, :, at].reshape(n_slot, step)) for f in range(n_blk))
            dy = dy_ref[:, at].astype(F32)
            mix = gate_ref[:, 0:1] * o_one + gate_ref[:, 1:2] * o_two
            out_ref[:, at] = (base_ref[:, at].astype(F32) + mix).astype(out_ref.dtype)
            sum_one[...] += lane_sums(dy * o_one)
            sum_two[...] += lane_sums(dy * o_two)

        [col(j) for j in range(tile // step)]

        @pl.when(pl.program_id(0) == pl.num_programs(0) - 1)
        def _():
            for k, total in enumerate((sum_one, sum_two)):
                dg = jnp.sum(total[...], axis=1, keepdims=True)
                dg_ref[:, k:k + 1] = refs[n_blk + 4][:, k:k + 1] + dg if extra else dg

    tok = pl.BlockSpec((n_tok, tile), lambda j: (0, j))
    small = lambda n: pl.BlockSpec((n_tok, n), lambda j: (0, 0))
    return call(body, (d_model // tile,),
                [pl.BlockSpec((n_exp, cap, tile), lambda j: (0, 0, j))] * n_blk + [small(2 * n_blk), small(2), tok, tok]
                + [small(2)] * len(extra), [tok, small(2)],
                [jax.ShapeDtypeStruct((n_tok, d_model), BF16 if extra else F32), jax.ShapeDtypeStruct((n_tok, 2), F32)],
                (*blocks, pos, gates, base, tok_dy, *extra), 4 * n_tok * n_blk * n_slot * d_model,
                [pltpu.VMEM((n_blk, n_tok, n_slot), BF16)] * 2 + [pltpu.VMEM((n_tok, 128), F32)] * 2)


def pair_hot(hot_ref, pos_ref, n_blk, n_slot):
    ids = lax.broadcasted_iota(jnp.int32, (pos_ref.shape[0], n_slot), 1)
    for f in range(n_blk):
        hit = (ids == pos_ref[:, f:f + 1]) | (ids == pos_ref[:, n_blk + f:n_blk + f + 1])
        hot_ref[f] = hit.astype(F32).astype(BF16)


def combine_part(blocks, pos):
    n_blk = len(blocks)
    n_exp, cap, d_model = blocks[0].shape
    n_tok, tile, step = pos.shape[0], 512, 256
    n_slot = n_exp * cap

    def body(*refs):
        blk, (pos_ref, out_ref, hot_ref) = refs[:n_blk], refs[n_blk:]

        @pl.when(pl.program_id(0) == 0)
        def _():
            pair_hot(hot_ref, pos_ref, n_blk, n_slot)

        def col(j):
            at = pl.ds(j * step, step)
            out_ref[:, at] = sum(mm(hot_ref[f], blk[f][:, :, at].reshape(n_slot, step)) for f in range(n_blk))

        [col(j) for j in range(tile // step)]

    return call(body, (d_model // tile,),
                [pl.BlockSpec((n_exp, cap, tile), lambda j: (0, 0, j))] * n_blk + [pl.BlockSpec((n_tok, 2 * n_blk), lambda j: (0, 0))],
                pl.BlockSpec((n_tok, tile), lambda j: (0, j)), jax.ShapeDtypeStruct((n_tok, d_model), F32),
                (*blocks, pos), 2 * n_tok * n_blk * n_slot * d_model, [pltpu.VMEM((n_blk, n_tok, n_slot), BF16)])


def combine_back(blocks, pos, part, tok_x, tok_dy, stats, d_logits, router, ln_weight):
    n_blk = len(blocks)
    n_exp, cap, d_model = blocks[0].shape
    n_tok, tile, step = tok_x.shape[0], 512, 256
    n_slot, n_tile = n_exp * cap, d_model // 512

    def body(*refs):
        blk = refs[:n_blk]
        (pos_ref, part_ref, x_ref, dy_ref, stat_ref, dl_ref, rt_ref, lnw_ref,
         dx_ref, dw_ref, db_ref, hot_ref, gh_ref, s1_ref, s2_ref, m1_ref, m2_ref) = refs[n_blk:]
        phase, j = pl.program_id(0), pl.program_id(1)

        @pl.when((phase == 0) & (j == 0))
        def _():
            s1_ref[...] = jnp.zeros_like(s1_ref)
            s2_ref[...] = jnp.zeros_like(s2_ref)
            pair_hot(hot_ref, pos_ref, n_blk, n_slot)

        @pl.when(phase == 0)
        def _():
            def col(i):
                at = pl.ds(i * step, step)
                grad = sum(mm(hot_ref[f], blk[f][:, :, at].reshape(n_slot, step)) for f in range(n_blk))
                grad = mm(dl_ref[...], rt_ref[:, at]) + (part_ref[:, at] + grad)
                gh_ref[j, :, at] = grad
                x_hat = (x_ref[:, at].astype(F32) - stat_ref[:, 0:1]) * stat_ref[:, 1:2]
                scaled = grad * lnw_ref[:, at].astype(F32)
                s1_ref[...] += lane_sums(scaled)
                s2_ref[...] += lane_sums(scaled * x_hat)
                dw_ref[:, at] = jnp.sum(grad * x_hat, axis=0, keepdims=True)
                db_ref[:, at] = jnp.sum(grad, axis=0, keepdims=True)

            [col(i) for i in range(tile // step)]

        @pl.when((phase == 1) & (j == 0))
        def _():
            m1_ref[...] = jnp.sum(s1_ref[...], axis=1, keepdims=True) / d_model
            m2_ref[...] = jnp.sum(s2_ref[...], axis=1, keepdims=True) / d_model

        @pl.when(phase == 1)
        def _():
            x_hat = (x_ref[...].astype(F32) - stat_ref[:, 0:1]) * stat_ref[:, 1:2]
            scaled = gh_ref[j] * lnw_ref[...].astype(F32)
            d_ln = stat_ref[:, 1:2] * (scaled - m1_ref[...] - x_hat * m2_ref[...])
            dx_ref[...] = (dy_ref[...].astype(F32) + d_ln).astype(BF16)

    last = n_tile - 1
    early = lambda p, j: j * (1 - p) + last * p
    tok = pl.BlockSpec((n_tok, tile), lambda p, j: (0, j))
    tok_early = pl.BlockSpec((n_tok, tile), lambda p, j: (0, early(p, j)))
    tok_late = pl.BlockSpec((n_tok, tile), lambda p, j: (0, j * p))
    wide = lambda n: pl.BlockSpec((n, tile), lambda p, j: (0, j))
    wide_early = lambda n: pl.BlockSpec((n, tile), lambda p, j: (0, early(p, j)))
    small = lambda n: pl.BlockSpec((n_tok, n), lambda p, j: (0, 0))
    return call(body, (2, n_tile),
                [pl.BlockSpec((n_exp, cap, tile), lambda p, j: (0, 0, early(p, j)))] * n_blk
                + [small(2 * n_blk), tok_early, tok, tok_late, small(2), small(router.shape[0]), wide(router.shape[0]), wide(1)],
                [tok_late, wide_early(1), wide_early(1)],
                [jax.ShapeDtypeStruct((n_tok, d_model), BF16)] + [jax.ShapeDtypeStruct((1, d_model), F32)] * 2,
                (*blocks, pos, part, tok_x, tok_dy, stats, d_logits, router, ln_weight), 2 * n_tok * n_blk * n_slot * d_model,
                [pltpu.VMEM((n_blk, n_tok, n_slot), BF16), pltpu.VMEM((n_tile, n_tok, tile), F32)]
                + [pltpu.VMEM((n_tok, 128), F32)] * 2 + [pltpu.VMEM((n_tok, 1), F32)] * 2)


FLIPS = {'x': (0, 2), 'y': (1, 0), 'c': (0, 1), 'd': (0, 3)}


def solution(mesh):
    n_dp, n_ep = mesh.shape['dp'], mesh.shape['ep']
    tok_spec = P(('dp', 'ep'), None)
    row_spec = P(('dp', 'ep'))
    exp_spec = P('ep', None, None)

    def swap(name, value, flips=None):
        flip_dp, flip_ep = flips or FLIPS[name[-1]]
        pairs = [(d * n_ep + e, (d ^ flip_dp) * n_ep + (e ^ flip_ep)) for d in range(n_dp) for e in range(n_ep)]
        return lax.ppermute(value, ('dp', 'ep'), pairs)

    def local_step(tok_x, tok_dy, exp_first, exp_second, eligible, slot_first, slot_second,
                   ln_weight, ln_bias, router, w_gate, w_up, w_down):
        n_local, d_model = tok_x.shape
        n_exp = eligible.shape[1]
        local_exp = w_gate.shape[0]
        cap = 3 * n_local // n_exp
        n_slot = local_exp * cap
        me = lax.axis_index('ep')
        weights = (jnp.swapaxes(w_gate, 1, 2), jnp.swapaxes(w_up, 1, 2), w_down)

        x_float = tok_x.astype(F32)
        mean = jnp.mean(x_float, axis=-1, keepdims=True)
        centered = x_float - mean
        inv_std = lax.rsqrt(jnp.mean(centered * centered, axis=-1, keepdims=True) + LN_EPS)
        hidden = (centered * inv_std * ln_weight.astype(F32) + ln_bias.astype(F32)).astype(BF16)
        logits = jnp.dot(hidden, router, preferred_element_type=F32)
        expert_ids = jnp.arange(n_exp)
        allowed = eligible > 0
        gate_one, prob_one, pick_one = masked_gate(logits, allowed, exp_first)
        gate_two, prob_two, pick_two = masked_gate(logits, allowed & (expert_ids[None, :] != exp_first[:, None]), exp_second)
        pos_one = jnp.where(slot_first >= 0, exp_first * cap + slot_first, -1)
        pos_two = jnp.where(slot_second >= 0, exp_second * cap + slot_second, -1)
        row_ids = jnp.arange(n_exp * cap)
        hit_one = pos_one[:, None] == row_ids[None, :]
        hit_two = pos_two[:, None] == row_ids[None, :]
        slot_tok = jnp.max(jnp.where(hit_one | hit_two, jnp.arange(n_local)[:, None], -1), axis=0).astype(F32)
        slot_gate = jnp.sum(jnp.where(hit_one, gate_one[:, None], 0.0) + jnp.where(hit_two, gate_two[:, None], 0.0), axis=0)
        meta = jnp.stack([slot_tok, slot_gate])

        def columns(*tables):
            mine = [lax.dynamic_slice(t, (0, me * n_slot), (2, n_slot)) for t in tables]
            both = jnp.stack(mine, axis=-1)
            return both[0].astype(jnp.int32), both[1]

        def spread(name, value):
            from_x = swap(name + '_x', value)
            from_y = swap(name + '_y', value)
            from_d = swap(name + '_xy', from_x)
            return [(v, swap(name + end, v)) for v, end in
                    ((value, '_c'), (from_x, '_xc'), (from_y, '_yc'), (from_d, '_dc'))]

        (m_a, m_x, m_y, m_d) = spread('m', meta)
        (h_a, h_x, h_y, h_d) = spread('h', hidden)
        first = spread('f', tok_dy[:, :512])
        rest = spread('g', tok_dy[:, 512:])
        g_a, g_x, g_y, g_d = ([(f, g) for f, g in zip(*both)] for both in zip(first, rest))
        h_a, h_x, h_y, h_d = ([(v,) for v in both] for both in (h_a, h_x, h_y, h_d))

        def gath(name, toks, tables):
            tab, gts = columns(*tables)
            return gather_rows(toks, tab, gts if name[-1] == 'q' else None, local_exp, cap)

        ha, qa = [gath('a_gath', h_a, m_a)], [gath('a_gq', g_a, m_a)]
        act_a, (ut_a, gt_a, vt_a), _ = up_pass(ha, qa, weights)
        o_a0, o_a1, b_a0, b_a1 = down_pass(*act_a, weights, cap, (0, 1))
        m_p, m_r = (m_x[0], m_y[0]), (m_x[1], m_y[1])
        hxy = [gath('p_gh', (h_x[0], h_y[0]), m_p), gath('r_gh', (h_x[1], h_y[1]), m_r)]
        (u_xy,), (ut_xy,), slopes = up_pass(hxy, None, weights)
        o_x0, o_x1 = down_pass(u_xy, None, None, weights, cap, (0, 2))
        qxy = [gath('p_gq', (g_x[0], g_y[0]), m_p), gath('r_gq', (g_x[1], g_y[1]), m_r)]
        d_xy, (gt_xy, vt_xy), _ = up_pass(None, qxy, weights, slopes)
        b_x0, b_x1 = down_pass(None, *d_xy, weights, cap, (0, 2))
        part, = weight_grads([((vt_xy, vt_a), hxy + ha, None)], 1024)
        hd = [gath('d%d_gh' % i, h_d[i:i + 1], m_d[i:i + 1]) for i in range(2)]
        _, (ut_d,), slopes = up_pass(hd, None, weights, plain=False)
        whole, qd = (local_exp, 2 * cap, d_model), None
        cols_d = [columns(m_d[0]), columns(m_d[1]), columns(*m_d)]
        stats = jnp.concatenate([mean, inv_std], axis=1)
        for i in range(2):
            qd = gather_rows([g_d[i][1:]], *cols_d[i], local_exp, cap, qd, whole, i, 1)
        du = late_pass(qd, w_down, 512)
        qd = gather_rows([g[:1] for g in g_d], *cols_d[2], local_exp, cap, qd, whole, after=du)
        gt_d, vt_d = late_pass(qd, w_down, 512, slopes, du)
        qd = [qd]
        dw_down, dw_gate, dw_up = weight_grads([
            ((ut_xy, ut_a, ut_d), qxy + qa + qd, None),
            ((gt_xy, gt_a, gt_d), hxy + ha + hd, None),
            ((vt_d,), hd, part)], 512)

        outs = [o_a0, swap('o_c', o_a1), swap('o_x', o_x0), swap('o_d', o_x1)]
        backs = [b_a0, swap('b_c', b_a1), swap('b_x', b_x0), swap('b_d', b_x1)]

        def slots(flips):
            cols = [(p, p - (me ^ f) * n_slot) for p in (pos_one, pos_two) for f in flips]
            return jnp.stack([jnp.where(p < 0, -1, at) for p, at in cols], axis=-1)

        near, far = slots((0, 1)), slots((2, 3))
        gates = jnp.stack([gate_one, gate_two], axis=-1)
        mix, dgate = combine_out(outs[:2], near, gates, tok_x, tok_dy)
        out_tok, dgate = combine_out(outs[2:], far, gates, mix, tok_dy, dgate)
        d_logits = ((dgate[:, 0] * gate_one)[:, None] * (pick_one - prob_one)
                    + (dgate[:, 1] * gate_two)[:, None] * (pick_two - prob_two)).astype(BF16)
        d_router = jnp.einsum('te,td->ed', d_logits, hidden, preferred_element_type=F32)

        def sum_all(name, value):
            for end in ('_c', '_y', '_x'):
                value = value + swap(name + end, value)
            return value

        d_router = sum_all('r', d_router)
        part_back = combine_part(backs[:2], near)
        dx_tok, d_lnw, d_lnb = combine_back(backs[2:], far, part_back, tok_x, tok_dy,
                                            stats, d_logits, router.T, ln_weight[None, :])
        d_ln = jnp.concatenate([d_lnw, d_lnb], axis=0)
        terms = [d_ln] + [swap('l%d' % f, d_ln, divmod(f, n_ep)) for f in range(1, n_dp * n_ep)]
        while len(terms) > 1:
            terms = [a + b for a, b in zip(terms[::2], terms[1::2])]
        d_ln = terms[0]
        return (out_tok, dx_tok, jnp.swapaxes(dw_gate, 1, 2), jnp.swapaxes(dw_up, 1, 2), dw_down, d_router.T, d_ln[0], d_ln[1])

    return jax.shard_map(
        local_step, mesh=mesh,
        in_specs=(tok_spec, tok_spec, row_spec, row_spec, tok_spec, row_spec, row_spec,
                  P(), P(), P(), exp_spec, exp_spec, exp_spec),
        out_specs=(tok_spec, tok_spec, exp_spec, exp_spec, exp_spec, P(), P(), P()),
        check_vma=False)
```
